32 devices in a mesh: groups: 2 (over y), range: 8 (over z, x), sub: 2 (over core).
Axes of the slice: x: 2, y: 2, z: 4, core: 2. Of those that a mesh axis runs over, the one named last changes fastest.
Arguments:
- samples: float32 [2, 1024, 32, 128], P(None, ('groups', 'range', 'sub')), parts along dimension 1, may hold values from -6 to 6
- beam_weights: float32 [32, 8, 2, 64, 128], P(('groups', 'range'), None, None, None, 'sub'), parts along dimension 0, may hold values from -0.25 to 0.25
- subarrays: int32 [32, 8, 64], P(('groups', 'range', 'sub')), parts along dimension 0, may hold values from 0 to 511, as said below
- training: int32 [64], P(('groups', 'range', 'sub')), parts along dimension 0, may hold values 0 or 1
Outputs:
- covariance: float32 [32, 8, 64, 128], P(('groups', 'range', 'sub')), parts along dimension 0
- filtered: float32 [2, 128, 64, 128], P(None, None, ('groups', 'range', 'sub')), parts along dimension 2
- energy: float32 [256], P('groups'), parts along dimension 0
The draws below stay inside these ranges and needn't reach their ends.
There are 2 independent parts, one for each index of `groups`. The reference program is written for one: setup_inputs(seed, part) draws one part's arguments, and reference() takes and returns one part's arrays. A program takes and returns all parts, laid end to end along the dimension named above; each array names one. Nothing has to cross between parts.
Inputs may be any that keep to these rules, and one draw needn't show every extreme that they name: `subarrays`: in each gate block the 512 indices are all 512 channels, each once.
All inputs are finite; a program needn't handle non-finite values. No bound on the sum of `training` on one device may be relied on, other than what follows from the above.
Results may differ from the reference program's by a relative error of at most 0.0003.
Values sent between devices are 32-bit elements; how exact they have to be, the bound alone decides.
No kernel may reach another device: no remote copies, remote signals or barrier semaphores. Data moves between devices by JAX's collectives and lax.ppermute only.
A program may use at most 64 MiB of HBM per device.

```python
import jax
import jax.numpy as jnp
from jax import lax

C = 512
S = 64
K = 128
P_SIZE = 128
GB = 2
NS = 8
G = 32
NB = 16


def draw_subarrays(key, part):
    several = jax.random.split(jax.random.fold_in(key, 17), NB)
    orders = jax.vmap(lambda single: jax.random.permutation(single, C))(several)
    return orders.reshape(NB, NS, S).astype(jnp.int32)


def plant(values, stream_key, smallest, top_value):
    longest = values.shape.index(max(values.shape))
    spots = []
    for shift in (0, 1):
        where = [jax.random.randint(jax.random.fold_in(stream_key, axis), (), 0, length) for axis, length in enumerate(values.shape)]
        where[longest] = (where[longest] + shift) % values.shape[longest]
        spots.append(tuple(where))
    return values.at[spots[0]].set(smallest).at[spots[1]].set(top_value)


def level_of(rng, extent, cuts, least, high):
    level, own = 1.0, jax.random.fold_in(rng, 6)
    for dim, parts in cuts:
        heights = jnp.exp(jax.random.uniform(jax.random.fold_in(own, dim), (parts,), jnp.float32, least / len(cuts), high / len(cuts)))
        level = level * jnp.repeat(heights, extent[dim] // parts).reshape([-1 if axis == dim else 1 for axis in range(len(extent))])
    return level


def normal_values(key, extent, width, bound, cuts=(), kind=jnp.bfloat16):
    drawn = width * jax.random.normal(key, extent, jnp.float32)
    if cuts:
        drawn = drawn * level_of(key, extent, cuts, -0.22, 0.18)
    return jnp.clip(drawn, -bound, bound).astype(kind)


def setup_inputs(seed: int = 0, part: int = 0) -> dict:
    splits = jax.random.split(jax.random.key(seed), 5)
    part_keys = jax.random.split(jax.random.fold_in(splits[4], part), 5)
    samples = normal_values(part_keys[0], (2, C, G, P_SIZE), 1.0, 6.0, ((1, 16),), jnp.float32)
    beam_weights = normal_values(part_keys[1], (NB, NS, 2, S, K), C ** -0.5, 0.25, ((0, 8), (4, 2)), jnp.float32)
    subarrays = draw_subarrays(jax.random.fold_in(jax.random.fold_in(splits[4], part), 71), part)
    training = plant((jax.random.randint(part_keys[3], (G,), 0, 2) < 1).astype(jnp.int32), jax.random.fold_in(part_keys[3], 1), 0, 1)
    return dict(samples=samples, beam_weights=beam_weights, subarrays=subarrays, training=training)


loading = 0.05

def block_terms(snaps, chosen, weights, masked, factor):
    highest = lax.Precision.HIGHEST
    picked = jnp.take(snaps, chosen, axis=1)
    real_part = picked[0]
    imag_part = picked[1]
    real_masked = real_part * masked
    imag_masked = imag_part * masked
    cov_real = (jnp.einsum('snx,smx->snm', real_masked, real_part, precision=highest) + jnp.einsum('snx,smx->snm', imag_masked, imag_part, precision=highest)) * factor
    cov_imag = (jnp.einsum('snx,smx->snm', imag_masked, real_part, precision=highest) - jnp.einsum('snx,smx->snm', real_masked, imag_part, precision=highest)) * factor
    w_real = weights[:, 0]
    w_imag = weights[:, 1]
    out_real = jnp.einsum('snk,snx->kx', w_real, real_part, precision=highest) + jnp.einsum('snk,snx->kx', w_imag, imag_part, precision=highest)
    out_imag = jnp.einsum('snk,snx->kx', w_real, imag_part, precision=highest) - jnp.einsum('snk,snx->kx', w_imag, real_part, precision=highest)
    prod_real = jnp.einsum('snm,smk->snk', cov_real, w_real, precision=highest) - jnp.einsum('snm,smk->snk', cov_imag, w_imag, precision=highest)
    prod_imag = jnp.einsum('snm,smk->snk', cov_real, w_imag, precision=highest) + jnp.einsum('snm,smk->snk', cov_imag, w_real, precision=highest)
    quadratic = lax.optimization_barrier(jnp.sum(w_real * prod_real + w_imag * prod_imag, axis=(0, 1)))
    inverse = 1.0 / jnp.sqrt(quadratic + loading)
    filtered = jnp.stack([out_real * inverse[:, None], out_imag * inverse[:, None]])
    energy = lax.optimization_barrier(jnp.sum(out_real * out_real + out_imag * out_imag, axis=1))
    covariance = jnp.concatenate([cov_real, cov_imag], axis=-1)
    return (covariance, filtered, energy)

def reference(samples, beam_weights, subarrays, training):
    factor = 1.0 / (GB * P_SIZE)

    def one_block(index):
        start = (index * GB).astype(jnp.int32)
        snaps = lax.dynamic_slice_in_dim(samples, start, GB, 2).reshape(2, C, GB * P_SIZE)
        gates_on = lax.dynamic_slice_in_dim(training, start, GB, 0).astype(jnp.float32)
        masked = jnp.repeat(gates_on, P_SIZE)
        return block_terms(snaps, subarrays[index], beam_weights[index], masked, factor)
    covs, filts, energies = lax.map(one_block, jnp.arange(NB, dtype=jnp.int32))
    filtered = filts.reshape(NB, 2, K, GB, P_SIZE).transpose(1, 2, 0, 3, 4).reshape(2, K, G, P_SIZE)
    energy = lax.optimization_barrier(jnp.sum(energies, axis=0)) / (G * P_SIZE)
    return (covs, filtered, energy)
```

```python
import functools

import jax
import jax.numpy as jnp
from jax import lax
from jax.experimental import pallas as pl
from jax.experimental.pallas import tpu as pltpu
from jax.sharding import PartitionSpec as P

GB = 2
AXES = ("range", "sub")

loading = 0.05


def split(value):
    high = value.astype(jnp.bfloat16)
    low = (value - high.astype(jnp.float32)).astype(jnp.bfloat16)
    return high, low


def dot(lhs, rhs, dims):
    return lax.dot_general(lhs, rhs, (dims, ((), ())), preferred_element_type=jnp.float32)


def dot3(lhs, rhs, dims):
    (lh, ll), (rh, rl) = lhs, rhs
    return dot(lh, rh, dims) + (dot(lh, rl, dims) + dot(ll, rh, dims))


def local_kernel(core, gates, turned, own, got, chosen, cov_out, filt_out, energy_out, *, factor):
    sources, rows, pulses = turned.shape
    subs, _, size, half = own.shape[1:]
    beams = 2 * half
    chan_dev = rows // (2 * GB)
    channels = sources * chan_dev
    flat = turned.reshape(sources * rows, pulses)

    columns = []
    for iq in range(2):
        for gate in range(GB):
            pieces = [
                flat[pl.ds(src * rows + iq * chan_dev * GB + gate, chan_dev, stride=GB), :]
                for src in range(sources)
            ]
            columns.append(jnp.concatenate(pieces, axis=0))
    snaps = jnp.concatenate(columns, axis=1)
    snap_high, snap_low = split(snaps)
    wanted = chosen[...]
    hot = (wanted == lax.broadcasted_iota(jnp.int32, (subs * size, channels), 1)).astype(jnp.bfloat16)
    rows_of = ((1,), (0,))
    pick_high = dot(hot, snap_high, rows_of).astype(jnp.bfloat16)
    pick_low = dot(hot, snap_low, rows_of).astype(jnp.bfloat16)

    first = core[0] == 0
    mine = own[0]
    other = got[...]
    low_half = jnp.where(first, mine, other)
    high_half = jnp.where(first, other, mine)
    both = jnp.concatenate([low_half, high_half], axis=-1)
    w_real = both[:, 0].reshape(subs * size, beams)
    w_imag = both[:, 1].reshape(subs * size, beams)
    weights = jnp.concatenate([w_real, w_imag], axis=1)
    wt_high, wt_low = split(weights)

    over_rows = ((0,), (0,))
    mixed = dot3((wt_high, wt_low), (pick_high, pick_low), over_rows)
    width = GB * pulses
    out_real = mixed[:beams, :width] + mixed[beams:, width:]
    out_imag = mixed[:beams, width:] - mixed[beams:, :width]
    power = out_real * out_real + out_imag * out_imag
    folded = power[:, :pulses]
    for gate in range(1, GB):
        folded = folded + power[:, gate * pulses:(gate + 1) * pulses]
    total = jnp.sum(folded.T, axis=0, keepdims=True)
    energy_out[...] = jnp.broadcast_to(total, energy_out.shape)

    column_gate = lax.broadcasted_iota(jnp.int32, (1, 2 * width), 1) // pulses % GB
    mask = jnp.zeros((1, 2 * width), jnp.float32)
    for gate in range(GB):
        mask = jnp.where(column_gate == gate, gates[gate].astype(jnp.float32), mask)
    mask = mask.astype(jnp.bfloat16)
    over_cols = ((1,), (1,))
    power_sum = jnp.zeros((size, beams), jnp.float32)
    for s in range(subs):
        part = slice(s * size, (s + 1) * size)
        zh, zl = pick_high[part], pick_low[part]
        right = [
            jnp.concatenate([z, jnp.concatenate([-z[:, width:], z[:, :width]], axis=1)], axis=0)
            for z in (zh, zl)
        ]
        cov = dot3((zh * mask, zl * mask), right, over_cols) * factor
        cov_out[0, s] = cov
        ws_high, ws_low = wt_high[part], wt_low[part]
        stacked = [
            jnp.concatenate([w, jnp.concatenate([-w[:, beams:], w[:, :beams]], axis=1)], axis=0)
            for w in (ws_high, ws_low)
        ]
        prod = dot3(split(cov), stacked, rows_of)
        terms = prod * weights[part]
        power_sum = power_sum + (terms[:, :beams] + terms[:, beams:])
    quadratic = jnp.sum(power_sum, axis=0, keepdims=True)
    inverse = 1.0 / jnp.sqrt(quadratic + loading)
    scale = jnp.broadcast_to(inverse, (pulses, beams)).T
    for iq, value in enumerate((out_real, out_imag)):
        for gate in range(GB):
            filt_out[iq, pl.ds(gate, beams, stride=GB), :] = value[:, gate * pulses:(gate + 1) * pulses] * scale


def body(samples, beam_weights, subarrays, training):
    range_count = lax.axis_size("range")
    core_count = lax.axis_size("sub")
    parts_iq, chan_dev, all_gates, pulses = samples.shape
    devices = range_count * core_count
    gate_dev = all_gates // devices
    subs, _, size, half = beam_weights.shape[1:]
    beams = half * core_count
    channels = chan_dev * devices
    core = lax.axis_index("sub")

    rows = parts_iq * chan_dev * gate_dev
    spread = samples.reshape(parts_iq, chan_dev, devices, gate_dev, pulses).transpose(2, 0, 1, 3, 4)
    spread = spread.reshape(devices, rows, pulses)
    turned = lax.all_to_all(spread, AXES, 0, 0, tiled=True)
    sent = lax.dynamic_index_in_dim(beam_weights, 1 - core, 0, keepdims=False)
    got = lax.ppermute(sent, "sub", [(0, 1), (1, 0)])

    factor = 1.0 / (GB * pulses)
    vmem = pl.BlockSpec(memory_space=pltpu.VMEM)
    whole = lambda shape: pl.BlockSpec(shape, lambda i, core, gates: (0,) * len(shape))
    out_shapes = (
        jax.ShapeDtypeStruct((1, subs, size, 2 * size), jnp.float32),
        jax.ShapeDtypeStruct((parts_iq, beams * gate_dev, pulses), jnp.float32),
        jax.ShapeDtypeStruct((devices, beams), jnp.float32),
    )
    covs, filts, energies = pl.pallas_call(
        functools.partial(local_kernel, factor=factor),
        out_shape=out_shapes,
        grid_spec=pltpu.PrefetchScalarGridSpec(
            num_scalar_prefetch=2,
            grid=(1,),
            in_specs=[
                whole((devices, rows, pulses)),
                pl.BlockSpec((1, subs, 2, size, half), lambda i, core, gates: (core[0], 0, 0, 0, 0)),
                whole((subs, 2, size, half)),
                whole((subs * size, 1)),
            ],
            out_specs=[whole(o.shape) for o in out_shapes],
        ),
    )(core.reshape(1).astype(jnp.int32), training, turned, beam_weights, got, subarrays.reshape(subs * size, 1))
    filtered = filts.reshape(parts_iq, beams, gate_dev, pulses)
    shared = lax.all_to_all(energies, AXES, 0, 0, tiled=True)
    energy = jnp.sum(shared, axis=0) * (1.0 / (all_gates * pulses))
    return (covs, filtered, energy)


def solution(mesh):
    placed = (
        P(None, ("groups", "range", "sub"), None, None),
        P(("groups", "range"), None, None, None, "sub"),
        P(("groups", "range", "sub"), None, None),
        P(("groups", "range", "sub")),
    )
    return jax.shard_map(
        body,
        mesh=mesh,
        in_specs=placed,
        out_specs=(
            P(("groups", "range", "sub"), None, None, None),
            P(None, None, ("groups", "range", "sub"), None),
            P("groups"),
        ),
        check_vma=False,
    )
```

```python
import functools

import jax
import jax.numpy as jnp
from jax import lax
from jax.experimental import pallas as pl
from jax.experimental.pallas import tpu as pltpu
from jax.sharding import PartitionSpec as P

GB = 2
AXES = ("range", "sub")
OVER_COLS_ROWS = ((1,), (0,))
OVER_ROWS = ((0,), (0,))
OVER_COLS = ((1,), (1,))

loading = 0.05

VMEM = pl.BlockSpec(memory_space=pltpu.VMEM)
SMEM = pl.BlockSpec(memory_space=pltpu.SMEM)


def split(value):
    high = value.astype(jnp.bfloat16)
    low = (value - high.astype(jnp.float32)).astype(jnp.bfloat16)
    return high, low


def dot(lhs, rhs, dims):
    return lax.dot_general(lhs, rhs, (dims, ((), ())), preferred_element_type=jnp.float32)


def dot3(lhs, rhs, dims):
    (lh, ll), (rh, rl) = lhs, rhs
    return dot(lh, rh, dims) + (dot(lh, rl, dims) + dot(ll, rh, dims))


def spread_kernel(samples, spread):
    parts_iq, chan_step, all_gates, pulses = samples.shape
    devices, rows, _ = spread.shape
    chan_dev = rows // (parts_iq * GB)
    flat = samples.reshape(parts_iq * chan_step * all_gates, pulses)
    start = pl.multiple_of(pl.program_id(0) * chan_step, chan_step)
    for iq in range(parts_iq):
        for gate in range(all_gates):
            dest, inner = divmod(gate, GB)
            row = iq * chan_step * all_gates + gate
            spread[dest, pl.ds((iq * GB + inner) * chan_dev + start, chan_step), :] = flat[
                pl.ds(row, chan_step, stride=all_gates), :
            ]


def prepare_kernel(core, own, got, chosen, hot_out, sub_out, chan_out):
    subs, _, size, half = got.shape
    beams = 2 * half
    channels = hot_out.shape[1]
    wanted = chosen[...]
    hot = (wanted == lax.broadcasted_iota(jnp.int32, (subs * size, channels), 1)).astype(jnp.bfloat16)
    hot_out[...] = hot
    mine = own[core[0]]
    other = got[...]
    first = core[0] == 0
    both = jnp.concatenate([jnp.where(first, mine, other), jnp.where(first, other, mine)], axis=-1)
    weights = jnp.concatenate([both[:, iq].reshape(subs * size, beams) for iq in range(2)], axis=1)
    for index, piece in enumerate(split(weights)):
        sub_out[index] = piece
        chan_out[index] = dot(hot, piece, OVER_ROWS).astype(jnp.bfloat16)


def beam_kernel(turned, weights, snap_out, beam_out, energy_out):
    sources, rows, pulses = turned.shape
    chan_dev = rows // (2 * GB)
    beams = weights.shape[2] // 2
    width = GB * pulses
    columns = [
        turned[:, piece * chan_dev:(piece + 1) * chan_dev, :].reshape(sources * chan_dev, pulses)
        for piece in range(2 * GB)
    ]
    snaps = split(jnp.concatenate(columns, axis=1))
    for index, piece in enumerate(snaps):
        snap_out[index] = piece
    mixed = dot3((weights[0], weights[1]), snaps, OVER_ROWS)
    out_real = mixed[:beams, :width] + mixed[beams:, width:]
    out_imag = mixed[:beams, width:] - mixed[beams:, :width]
    beam_out[0] = out_real
    beam_out[1] = out_imag
    power = out_real * out_real + out_imag * out_imag
    folded = power[:, :pulses]
    for gate in range(1, GB):
        folded = folded + power[:, gate * pulses:(gate + 1) * pulses]
    total = jnp.sum(folded.T, axis=0, keepdims=True)
    energy_out[...] = jnp.broadcast_to(total, energy_out.shape)


def covariance_kernel(gates, hot, snaps, weights, beam_in, cov_out, filt_out, *, factor):
    subs, size = cov_out.shape[1:3]
    beams = weights.shape[2] // 2
    width = beam_in.shape[2]
    pulses = width // GB
    picked = [dot(hot[...], snaps[index], OVER_COLS_ROWS).astype(jnp.bfloat16) for index in range(2)]
    column_gate = lax.broadcasted_iota(jnp.int32, (1, 2 * width), 1) // pulses % GB
    mask = jnp.zeros((1, 2 * width), jnp.float32)
    for gate in range(GB):
        mask = jnp.where(column_gate == gate, gates[gate].astype(jnp.float32), mask)
    mask = mask.astype(jnp.bfloat16)
    power_sum = jnp.zeros((size, beams), jnp.float32)
    for s in range(subs):
        part = slice(s * size, (s + 1) * size)
        rows = [z[part] for z in picked]
        right = [
            jnp.concatenate([z, jnp.concatenate([-z[:, width:], z[:, :width]], axis=1)], axis=0) for z in rows
        ]
        cov = dot3([z * mask for z in rows], right, OVER_COLS) * factor
        cov_out[0, s] = cov
        own = [weights[index, part] for index in range(2)]
        stacked = [
            jnp.concatenate([w, jnp.concatenate([-w[:, beams:], w[:, :beams]], axis=1)], axis=0) for w in own
        ]
        prod = dot3(split(cov), stacked, OVER_COLS_ROWS)
        terms = prod * (own[0].astype(jnp.float32) + own[1].astype(jnp.float32))
        power_sum = power_sum + (terms[:, :beams] + terms[:, beams:])
    quadratic = jnp.sum(power_sum, axis=0, keepdims=True)
    inverse = 1.0 / jnp.sqrt(quadratic + loading)
    scale = jnp.broadcast_to(inverse, (pulses, beams)).T
    for iq in range(2):
        for gate in range(GB):
            filt_out[iq, pl.ds(gate, beams, stride=GB), :] = (
                beam_in[iq, :, gate * pulses:(gate + 1) * pulses] * scale
            )


def near(array):
    return pltpu.with_memory_space_constraint(array, pltpu.VMEM)


def call(kernel, out_shape, in_specs, *operands):
    return pl.pallas_call(
        kernel,
        out_shape=out_shape,
        in_specs=in_specs,
        out_specs=(VMEM,) * len(out_shape),
    )(*operands)


def body(samples, beam_weights, subarrays, training):
    range_count = lax.axis_size("range")
    core_count = lax.axis_size("sub")
    parts_iq, chan_dev, all_gates, pulses = samples.shape
    devices = range_count * core_count
    gate_dev = all_gates // devices
    subs, _, size, half = beam_weights.shape[1:]
    beams = half * core_count
    channels = chan_dev * devices
    core = lax.axis_index("sub")
    single, half_type = jnp.float32, jnp.bfloat16
    shaped = jax.ShapeDtypeStruct

    rows = parts_iq * chan_dev * gate_dev
    chan_step = min(chan_dev, 8)
    spread = pl.pallas_call(
        spread_kernel,
        out_shape=shaped((devices, rows, pulses), single),
        grid=(chan_dev // chan_step,),
        in_specs=[pl.BlockSpec((parts_iq, chan_step, all_gates, pulses), lambda i: (0, i, 0, 0))],
        out_specs=VMEM,
    )(samples)
    turned = lax.all_to_all(spread, AXES, 0, 0, tiled=True)
    sent = lax.dynamic_index_in_dim(beam_weights, 1 - core, 0, keepdims=False)
    got = lax.ppermute(sent, "sub", [(0, 1), (1, 0)])
    hot, sub_weights, chan_weights = call(
        prepare_kernel,
        (
            shaped((channels, channels), half_type),
            shaped((2, channels, 2 * beams), half_type),
            shaped((2, channels, 2 * beams), half_type),
        ),
        [SMEM, VMEM, VMEM, VMEM],
        core.reshape(1).astype(jnp.int32),
        near(beam_weights),
        near(got),
        near(subarrays.reshape(subs * size, 1)),
    )
    snaps, outs, energies = call(
        beam_kernel,
        (
            shaped((2, channels, parts_iq * gate_dev * pulses), half_type),
            shaped((parts_iq, beams, gate_dev * pulses), single),
            shaped((devices, beams), single),
        ),
        [VMEM, VMEM],
        near(turned),
        chan_weights,
    )
    shared = lax.all_to_all(energies, AXES, 0, 0, tiled=True)
    covs, filts = call(
        functools.partial(covariance_kernel, factor=1.0 / (GB * pulses)),
        (
            shaped((1, subs, size, 2 * size), single),
            shaped((parts_iq, beams * gate_dev, pulses), single),
        ),
        [SMEM, VMEM, VMEM, VMEM, VMEM],
        training,
        hot,
        snaps,
        sub_weights,
        outs,
    )
    filtered = filts.reshape(parts_iq, beams, gate_dev, pulses)
    energy = jnp.sum(shared, axis=0) * (1.0 / (all_gates * pulses))
    return (covs, filtered, energy)


def solution(mesh):
    placed = (
        P(None, ("groups", "range", "sub"), None, None),
        P(("groups", "range"), None, None, None, "sub"),
        P(("groups", "range", "sub"), None, None),
        P(("groups", "range", "sub")),
    )
    return jax.shard_map(
        body,
        mesh=mesh,
        in_specs=placed,
        out_specs=(
            P(("groups", "range", "sub"), None, None, None),
            P(None, None, ("groups", "range", "sub"), None),
            P("groups"),
        ),
        check_vma=False,
    )
```

```python
import functools

import jax
import jax.numpy as jnp
from jax import lax
from jax.experimental import pallas as pl
from jax.experimental.pallas import tpu as pltpu
from jax.sharding import PartitionSpec as P

GB = 2
AXES = ("range", "sub")
OVER_COLS_ROWS = ((1,), (0,))
OVER_ROWS = ((0,), (0,))
OVER_COLS = ((1,), (1,))

loading = 0.05

VMEM = pl.BlockSpec(memory_space=pltpu.VMEM)
SMEM = pl.BlockSpec(memory_space=pltpu.SMEM)


def split(value):
    high = value.astype(jnp.bfloat16)
    low = (value - high.astype(jnp.float32)).astype(jnp.bfloat16)
    return high, low


def dot(lhs, rhs, dims):
    return lax.dot_general(lhs, rhs, (dims, ((), ())), preferred_element_type=jnp.float32)


def dot3(lhs, rhs, dims):
    (lh, ll), (rh, rl) = lhs, rhs
    return dot(lh, rh, dims) + (dot(lh, rl, dims) + dot(ll, rh, dims))


def spread_kernel(samples, spread):
    parts_iq, chan_step, all_gates, pulses = samples.shape
    flat = samples.reshape(parts_iq * chan_step * all_gates, pulses)
    for iq in range(parts_iq):
        for gate in range(all_gates):
            dest, inner = divmod(gate, GB)
            row = iq * chan_step * all_gates + gate
            spread[dest, iq * GB + inner] = flat[pl.ds(row, chan_step, stride=all_gates), :]


def snapshots(turned):
    sources, rows, pulses = turned.shape
    chan_dev = rows // (2 * GB)
    columns = [
        turned[:, piece * chan_dev:(piece + 1) * chan_dev, :].reshape(sources * chan_dev, pulses)
        for piece in range(2 * GB)
    ]
    return split(jnp.concatenate(columns, axis=1))


def prepare_kernel(core, own, got, chosen, hot_out, sub_out, chan_out):
    subs, _, size, half = got.shape
    beams = 2 * half
    channels = hot_out.shape[1]
    wanted = chosen[...]
    hot = (wanted == lax.broadcasted_iota(jnp.int32, (subs * size, channels), 1)).astype(jnp.bfloat16)
    hot_out[...] = hot
    mine = own[core[0]]
    other = got[...]
    first = core[0] == 0
    both = jnp.concatenate([jnp.where(first, mine, other), jnp.where(first, other, mine)], axis=-1)
    weights = jnp.concatenate([both[:, iq].reshape(subs * size, beams) for iq in range(2)], axis=1)
    for index, piece in enumerate(split(weights)):
        sub_out[index] = piece
        chan_out[index] = dot(hot, piece, OVER_ROWS).astype(jnp.bfloat16)


def beam_kernel(turned, weights, beam_out, energy_out):
    pulses = turned.shape[2]
    beams = weights.shape[2] // 2
    width = GB * pulses
    snaps = snapshots(turned)
    mixed = dot3((weights[0], weights[1]), snaps, OVER_ROWS)
    out_real = mixed[:beams, :width] + mixed[beams:, width:]
    out_imag = mixed[:beams, width:] - mixed[beams:, :width]
    beam_out[0] = out_real
    beam_out[1] = out_imag
    power = out_real * out_real + out_imag * out_imag
    folded = power[:, :pulses]
    for gate in range(1, GB):
        folded = folded + power[:, gate * pulses:(gate + 1) * pulses]
    total = jnp.sum(folded.T, axis=0, keepdims=True)
    energy_out[...] = jnp.broadcast_to(total, energy_out.shape)


def covariance_kernel(gates, hot, turned, weights, beam_in, cov_out, filt_out, *, factor):
    subs, size = cov_out.shape[1:3]
    beams = weights.shape[2] // 2
    width = beam_in.shape[2]
    pulses = width // GB
    picked = [dot(hot[...], piece, OVER_COLS_ROWS).astype(jnp.bfloat16) for piece in snapshots(turned)]
    column_gate = lax.broadcasted_iota(jnp.int32, (1, 2 * width), 1) // pulses % GB
    mask = jnp.zeros((1, 2 * width), jnp.float32)
    for gate in range(GB):
        mask = jnp.where(column_gate == gate, gates[gate].astype(jnp.float32), mask)
    mask = mask.astype(jnp.bfloat16)
    power_sum = jnp.zeros((size, beams), jnp.float32)
    for s in range(subs):
        part = slice(s * size, (s + 1) * size)
        rows = [z[part] for z in picked]
        right = [
            jnp.concatenate([z, jnp.concatenate([-z[:, width:], z[:, :width]], axis=1)], axis=0) for z in rows
        ]
        cov = dot3([z * mask for z in rows], right, OVER_COLS) * factor
        cov_out[0, s] = cov
        own = [weights[index, part] for index in range(2)]
        stacked = [
            jnp.concatenate([w, jnp.concatenate([-w[:, beams:], w[:, :beams]], axis=1)], axis=0) for w in own
        ]
        prod = dot3(split(cov), stacked, OVER_COLS_ROWS)
        terms = prod * (own[0].astype(jnp.float32) + own[1].astype(jnp.float32))
        power_sum = power_sum + (terms[:, :beams] + terms[:, beams:])
    quadratic = jnp.sum(power_sum, axis=0, keepdims=True)
    inverse = 1.0 / jnp.sqrt(quadratic + loading)
    scale = jnp.broadcast_to(inverse, (pulses, beams)).T
    for iq in range(2):
        for gate in range(GB):
            filt_out[iq, pl.ds(gate, beams, stride=GB), :] = (
                beam_in[iq, :, gate * pulses:(gate + 1) * pulses] * scale
            )


def near(array):
    return pltpu.with_memory_space_constraint(array, pltpu.VMEM)


def call(kernel, out_shape, in_specs, *operands):
    return pl.pallas_call(
        kernel,
        out_shape=out_shape,
        in_specs=in_specs,
        out_specs=(VMEM,) * len(out_shape),
    )(*operands)


def body(samples, beam_weights, subarrays, training):
    range_count = lax.axis_size("range")
    core_count = lax.axis_size("sub")
    parts_iq, chan_dev, all_gates, pulses = samples.shape
    devices = range_count * core_count
    gate_dev = all_gates // devices
    subs, _, size, half = beam_weights.shape[1:]
    beams = half * core_count
    channels = chan_dev * devices
    core = lax.axis_index("sub")
    single, half_type = jnp.float32, jnp.bfloat16
    shaped = jax.ShapeDtypeStruct

    rows = parts_iq * chan_dev * gate_dev
    chan_step = min(chan_dev, 8)
    spread = pl.pallas_call(
        spread_kernel,
        out_shape=shaped((devices, parts_iq * gate_dev, chan_dev, pulses), single),
        grid=(chan_dev // chan_step,),
        in_specs=[pl.BlockSpec((parts_iq, chan_step, all_gates, pulses), lambda i: (0, i, 0, 0))],
        out_specs=pl.BlockSpec((devices, parts_iq * gate_dev, chan_step, pulses), lambda i: (0, 0, i, 0)),
    )(samples).reshape(devices, rows, pulses)
    turned = near(lax.all_to_all(spread, AXES, 0, 0, tiled=True))
    sent = lax.dynamic_index_in_dim(beam_weights, 1 - core, 0, keepdims=False)
    got = lax.ppermute(sent, "sub", [(0, 1), (1, 0)])
    hot, sub_weights, chan_weights = call(
        prepare_kernel,
        (
            shaped((channels, channels), half_type),
            shaped((2, channels, 2 * beams), half_type),
            shaped((2, channels, 2 * beams), half_type),
        ),
        [SMEM, VMEM, VMEM, VMEM],
        core.reshape(1).astype(jnp.int32),
        near(beam_weights),
        near(got),
        near(subarrays.reshape(subs * size, 1)),
    )
    outs, energies = call(
        beam_kernel,
        (
            shaped((parts_iq, beams, gate_dev * pulses), single),
            shaped((devices, beams), single),
        ),
        [VMEM, VMEM],
        turned,
        near(chan_weights),
    )
    shared = lax.all_to_all(energies, AXES, 0, 0, tiled=True)
    covs, filts = call(
        functools.partial(covariance_kernel, factor=1.0 / (GB * pulses)),
        (
            shaped((1, subs, size, 2 * size), single),
            shaped((parts_iq, beams * gate_dev, pulses), single),
        ),
        [SMEM, VMEM, VMEM, VMEM, VMEM],
        training,
        near(hot),
        turned,
        near(sub_weights),
        outs,
    )
    filtered = filts.reshape(parts_iq, beams, gate_dev, pulses)
    energy = jnp.sum(shared, axis=0) * (1.0 / (all_gates * pulses))
    return (covs, filtered, energy)


def solution(mesh):
    placed = (
        P(None, ("groups", "range", "sub"), None, None),
        P(("groups", "range"), None, None, None, "sub"),
        P(("groups", "range", "sub"), None, None),
        P(("groups", "range", "sub")),
    )
    return jax.shard_map(
        body,
        mesh=mesh,
        in_specs=placed,
        out_specs=(
            P(("groups", "range", "sub"), None, None, None),
            P(None, None, ("groups", "range", "sub"), None),
            P("groups"),
        ),
        check_vma=False,
    )
```

```python
import functools

import jax
import jax.numpy as jnp
from jax import lax
from jax.experimental import pallas as pl
from jax.experimental.pallas import tpu as pltpu
from jax.sharding import PartitionSpec as P

GB = 2
AXES = ("range", "sub")
OVER_COLS_ROWS = ((1,), (0,))
OVER_ROWS = ((0,), (0,))
OVER_COLS = ((1,), (1,))

loading = 0.05

VMEM = pl.BlockSpec(memory_space=pltpu.VMEM)
SMEM = pl.BlockSpec(memory_space=pltpu.SMEM)


def split(value):
    high = value.astype(jnp.bfloat16)
    low = (value - high.astype(jnp.float32)).astype(jnp.bfloat16)
    return high, low


def dot(lhs, rhs, dims):
    return lax.dot_general(lhs, rhs, (dims, ((), ())), preferred_element_type=jnp.float32)


def dot3(lhs, rhs, dims):
    (lh, ll), (rh, rl) = lhs, rhs
    return dot(lh, rh, dims) + (dot(lh, rl, dims) + dot(ll, rh, dims))


def snapshots(turned):
    sources, rows, pulses = turned.shape
    chan_dev = rows // (2 * GB)
    flat = turned.reshape(sources * rows, pulses)
    columns = []
    for iq in range(2):
        for gate in range(GB):
            starts = [src * rows + iq * chan_dev * GB + gate for src in range(sources)]
            pieces = [flat[pl.ds(start, chan_dev, stride=GB), :] for start in starts]
            columns.append(jnp.concatenate(pieces, axis=0))
    return split(jnp.concatenate(columns, axis=1))


def prepare_kernel(core, own, got, chosen, hot_out, sub_out, chan_out):
    subs, _, size, half = got.shape
    beams = 2 * half
    channels = hot_out.shape[1]
    wanted = chosen[...]
    hot = (wanted == lax.broadcasted_iota(jnp.int32, (subs * size, channels), 1)).astype(jnp.bfloat16)
    hot_out[...] = hot
    mine = own[core[0]]
    other = got[...]
    first = core[0] == 0
    both = jnp.concatenate([jnp.where(first, mine, other), jnp.where(first, other, mine)], axis=-1)
    weights = jnp.concatenate([both[:, iq].reshape(subs * size, beams) for iq in range(2)], axis=1)
    for index, piece in enumerate(split(weights)):
        sub_out[index] = piece
        chan_out[index] = dot(hot, piece, OVER_ROWS).astype(jnp.bfloat16)


def beam_kernel(turned, weights, beam_out, energy_out):
    pulses = turned.shape[2]
    beams = weights.shape[2] // 2
    width = GB * pulses
    snaps = snapshots(turned)
    mixed = dot3((weights[0], weights[1]), snaps, OVER_ROWS)
    out_real = mixed[:beams, :width] + mixed[beams:, width:]
    out_imag = mixed[:beams, width:] - mixed[beams:, :width]
    beam_out[0] = out_real
    beam_out[1] = out_imag
    power = out_real * out_real + out_imag * out_imag
    folded = power[:, :pulses]
    for gate in range(1, GB):
        folded = folded + power[:, gate * pulses:(gate + 1) * pulses]
    total = jnp.sum(folded.T, axis=0, keepdims=True)
    energy_out[...] = jnp.broadcast_to(total, energy_out.shape)


def covariance_kernel(gates, hot, turned, weights, beam_in, cov_out, filt_out, *, factor):
    subs, size = cov_out.shape[1:3]
    beams = weights.shape[2] // 2
    width = beam_in.shape[2]
    pulses = width // GB
    picked = [dot(hot[...], piece, OVER_COLS_ROWS).astype(jnp.bfloat16) for piece in snapshots(turned)]
    column_gate = lax.broadcasted_iota(jnp.int32, (1, 2 * width), 1) // pulses % GB
    mask = jnp.zeros((1, 2 * width), jnp.float32)
    for gate in range(GB):
        mask = jnp.where(column_gate == gate, gates[gate].astype(jnp.float32), mask)
    mask = mask.astype(jnp.bfloat16)
    power_sum = jnp.zeros((size, beams), jnp.float32)
    for s in range(subs):
        part = slice(s * size, (s + 1) * size)
        rows = [z[part] for z in picked]
        right = [
            jnp.concatenate([z, jnp.concatenate([-z[:, width:], z[:, :width]], axis=1)], axis=0) for z in rows
        ]
        cov = dot3([z * mask for z in rows], right, OVER_COLS) * factor
        cov_out[0, s] = cov
        own = [weights[index, part] for index in range(2)]
        stacked = [
            jnp.concatenate([w, jnp.concatenate([-w[:, beams:], w[:, :beams]], axis=1)], axis=0) for w in own
        ]
        prod = dot3(split(cov), stacked, OVER_COLS_ROWS)
        terms = prod * (own[0].astype(jnp.float32) + own[1].astype(jnp.float32))
        power_sum = power_sum + (terms[:, :beams] + terms[:, beams:])
    quadratic = jnp.sum(power_sum, axis=0, keepdims=True)
    inverse = 1.0 / jnp.sqrt(quadratic + loading)
    scale = jnp.broadcast_to(inverse, (pulses, beams)).T
    for iq in range(2):
        for gate in range(GB):
            filt_out[iq, pl.ds(gate, beams, stride=GB), :] = (
                beam_in[iq, :, gate * pulses:(gate + 1) * pulses] * scale
            )


def near(array):
    return pltpu.with_memory_space_constraint(array, pltpu.VMEM)


def call(kernel, out_shape, in_specs, *operands):
    return pl.pallas_call(
        kernel,
        out_shape=out_shape,
        in_specs=in_specs,
        out_specs=(VMEM,) * len(out_shape),
    )(*operands)


def body(samples, beam_weights, subarrays, training):
    range_count = lax.axis_size("range")
    core_count = lax.axis_size("sub")
    parts_iq, chan_dev, all_gates, pulses = samples.shape
    devices = range_count * core_count
    gate_dev = all_gates // devices
    subs, _, size, half = beam_weights.shape[1:]
    beams = half * core_count
    channels = chan_dev * devices
    core = lax.axis_index("sub")
    single, half_type = jnp.float32, jnp.bfloat16
    shaped = jax.ShapeDtypeStruct

    rows = parts_iq * chan_dev * gate_dev
    spread = samples.reshape(parts_iq, chan_dev, devices, gate_dev, pulses).transpose(2, 0, 1, 3, 4)
    spread = spread.reshape(devices, rows, pulses)
    turned = near(lax.all_to_all(spread, AXES, 0, 0, tiled=True))
    sent = lax.dynamic_index_in_dim(beam_weights, 1 - core, 0, keepdims=False)
    got = lax.ppermute(sent, "sub", [(0, 1), (1, 0)])
    hot, sub_weights, chan_weights = call(
        prepare_kernel,
        (
            shaped((channels, channels), half_type),
            shaped((2, channels, 2 * beams), half_type),
            shaped((2, channels, 2 * beams), half_type),
        ),
        [SMEM, VMEM, VMEM, VMEM],
        core.reshape(1).astype(jnp.int32),
        near(beam_weights),
        near(got),
        near(subarrays.reshape(subs * size, 1)),
    )
    outs, energies = call(
        beam_kernel,
        (
            shaped((parts_iq, beams, gate_dev * pulses), single),
            shaped((devices, beams), single),
        ),
        [VMEM, VMEM],
        turned,
        chan_weights,
    )
    shared = lax.all_to_all(energies, AXES, 0, 0, tiled=True)
    covs, filts = call(
        functools.partial(covariance_kernel, factor=1.0 / (GB * pulses)),
        (
            shaped((1, subs, size, 2 * size), single),
            shaped((parts_iq, beams * gate_dev, pulses), single),
        ),
        [SMEM, VMEM, VMEM, VMEM, VMEM],
        training,
        near(hot),
        turned,
        near(sub_weights),
        outs,
    )
    filtered = filts.reshape(parts_iq, beams, gate_dev, pulses)
    energy = jnp.sum(shared, axis=0) * (1.0 / (all_gates * pulses))
    return (covs, filtered, energy)


def solution(mesh):
    placed = (
        P(None, ("groups", "range", "sub"), None, None),
        P(("groups", "range"), None, None, None, "sub"),
        P(("groups", "range", "sub"), None, None),
        P(("groups", "range", "sub")),
    )
    return jax.shard_map(
        body,
        mesh=mesh,
        in_specs=placed,
        out_specs=(
            P(("groups", "range", "sub"), None, None, None),
            P(None, None, ("groups", "range", "sub"), None),
            P("groups"),
        ),
        check_vma=False,
    )
```
